32 devices in a mesh: grp: 2 (over x), rep: 8 (over z, y), blk: 2 (over core).
Axes of the slice: x: 2, y: 2, z: 4, core: 2. Of those that a mesh axis runs over, the one named last changes fastest.
Arguments:
- factors: float32 [16, 1280, 1280], P('grp', ('blk', 'rep')), as said below
- damping: float32 [16], P('grp'), may hold values from 0.1 to 1
Outputs:
- root: float32 [16, 1280, 1280], P('grp', ('blk', 'rep'))
- inv_root: float32 [16, 1280, 1280], P('grp', ('blk', 'rep'))
The draws below stay inside these ranges and needn't reach their ends.
Inputs may be any that keep to these rules, and one draw needn't show every extreme that they name: `factors`: every factor is symmetric positive semidefinite.
All inputs are finite; a program needn't handle non-finite values.
Results may differ from the reference program's by a relative error of at most 0.0035.
The reference program's roundings to bfloat16 on the way (of `step_mat`) count: a program that leaves them out, or rounds other values in their place, can miss the bound.
Values may be sent and summed in bfloat16 or wider, within the bound.
A program may use at most 128 MiB of HBM per device.

```python
import math
import jax
import jax.numpy as jnp
from jax import lax

N = 1280
ITERS = 4
FACTORS = 16


def draw_factors(key, part):
    mix_key, scale_key = jax.random.split(jax.random.fold_in(key, 11))
    mixing = jax.random.normal(mix_key, (FACTORS, N, N), jnp.float32)
    spectrum = jnp.exp(jax.random.uniform(scale_key, (FACTORS, N), jnp.float32, jnp.log(0.001), jnp.log(10.0)))
    weighted = mixing * spectrum[:, None, :]
    product = jnp.einsum('fik,fjk->fij', weighted, mixing, precision=lax.Precision.HIGHEST) / N
    return 0.5 * (product + jnp.swapaxes(product, 1, 2))


def levels(rng, dims, pieces, least, top_value):
    def one(position, blocks):
        steps = jax.random.uniform(jax.random.fold_in(jax.random.fold_in(rng, 6), position), (blocks,), jnp.float32, least / len(pieces), top_value / len(pieces))
        return jnp.repeat(jnp.exp(steps), dims[position] // blocks).reshape((-1,) + (1,) * (len(dims) - position - 1))

    loudness = one(*pieces[0])
    for cut in pieces[1:]:
        loudness = loudness * one(*cut)
    return loudness


def setup_inputs(seed: int = 0) -> dict:
    key_of = jax.random.split(jax.random.key(seed), 3)
    factors = draw_factors(jax.random.fold_in(key_of[2], 71), 0)
    damping = jnp.clip(jnp.exp(math.log(1.0) - 2.3025851 * jax.random.uniform(key_of[1], (FACTORS,), jnp.float32) ** levels(key_of[1], (FACTORS,), ((0, 2),), -0.2, 0.2)), 0.1, 1.0)
    return dict(factors=factors, damping=damping)


def one_factor(factor_pair):
    factor, damp_value = factor_pair
    identity = jnp.eye(N, dtype=jnp.float32)
    damped = factor + damp_value * identity
    frob_norm = jnp.sqrt(jnp.sum(damped * damped))
    iterate = (damped / frob_norm).astype(jnp.bfloat16)
    inverse = identity.astype(jnp.bfloat16)
    for sweep_idx in range(ITERS):
        moment = jnp.dot(inverse, iterate, preferred_element_type=jnp.float32)
        step_mat = ((3.0 * identity - moment) * 0.5).astype(jnp.bfloat16)
        new_iterate = jnp.dot(iterate, step_mat, preferred_element_type=jnp.float32).astype(jnp.bfloat16)
        inverse = jnp.dot(step_mat, inverse, preferred_element_type=jnp.float32).astype(jnp.bfloat16)
        iterate = new_iterate
    root_scale = jnp.sqrt(frob_norm)
    return (iterate.astype(jnp.float32) * root_scale, inverse.astype(jnp.float32) / root_scale)

def reference(factors, damping):
    root, inv_root = lax.map(one_factor, (factors, damping))
    return (root, inv_root)
```

```python
import functools

import jax
import jax.numpy as jnp
from jax import lax
from jax.experimental import pallas as pl
from jax.experimental.pallas import tpu as pltpu
from jax.sharding import PartitionSpec as P

ITERS = 4
LANES = 128
CHUNK = 256
MESH = pl.DeviceIdType.MESH


def kernel(
    reps, fac_hbm, damp_ref,
    root_ref, inv_ref, norm_ref,
    fac, part, scale, send_buf, full, step, last_root,
    load_sem, sum_send, sum_recv, in_send, in_recv, fwd_send, fwd_recv,
    ex_send, ex_recv, root_send, root_recv, inv_send, inv_recv,
):
    grp = lax.axis_index("grp")
    rep = lax.axis_index("rep")
    blk = lax.axis_index("blk")
    facs, rows, order = fac.shape
    half = rows * reps
    members = 2 * reps
    rank = blk * reps + rep
    chunks = order // CHUNK
    f32, bf16 = jnp.float32, jnp.bfloat16

    def remote(src, dst, send, recv, r, b):
        return pltpu.make_async_remote_copy(
            src_ref=src, dst_ref=dst, send_sem=send, recv_sem=recv,
            device_id=(grp, r, b), device_id_type=MESH,
        )

    def member(j):
        q = lax.rem(rank + j, members)
        return lax.rem(q, reps), q // reps

    loads = [
        pltpu.make_async_copy(fac_hbm.at[f], fac.at[f], load_sem.at[f]) for f in range(facs)
    ]
    for load in loads:
        load.start()
    barrier = pltpu.get_barrier_semaphore()
    for j in range(1, members):
        r, b = member(j)
        pl.semaphore_signal(barrier, inc=1, device_id=(grp, r, b), device_id_type=MESH)

    row_ids = rank * rows + lax.broadcasted_iota(jnp.int32, (rows, order), 0)
    diag = row_ids == lax.broadcasted_iota(jnp.int32, (rows, order), 1)

    def damped(f):
        return fac[f] + jnp.where(diag, damp_ref[f], 0.0)

    for f in range(facs):
        loads[f].wait()
        x = damped(f)
        col = jnp.sum(x * x, axis=0, keepdims=True)
        acc = col[:, :LANES]
        for c in range(1, order // LANES):
            acc = acc + col[:, c * LANES : (c + 1) * LANES]
        part[pl.ds(rank, 1), f : f + 1, :] = acc[None]
    pl.semaphore_wait(barrier, members - 1)

    sums = []
    for j in range(1, members):
        r, b = member(j)
        copy = remote(part.at[rank], part.at[rank], sum_send.at[j], sum_recv.at[j], r, b)
        copy.start()
        sums.append(copy)
    for copy in sums:
        copy.wait()
    total = part[0]
    for q in range(1, members):
        total = total + part[q]
    norm = jnp.sqrt(jnp.sum(total, axis=1, keepdims=True))
    norm_ref[...] = jnp.broadcast_to(norm, norm_ref.shape)
    scale[...] = jnp.broadcast_to(1.0 / norm, scale.shape)

    y0, z1 = full.at[0], full.at[1]

    def block_rows(b, r):
        return pl.ds(pl.multiple_of((b * reps + r) * rows, rows), rows)

    ins = []
    for k in range(1, reps):
        p = lax.rem(rep + k, reps)
        send_buf[k] = (damped(p) * scale[pl.ds(p, 1), 0:1]).astype(bf16)
        copy = remote(
            send_buf.at[k], y0.at[block_rows(blk, rep)], in_send.at[k], in_recv.at[k], p, blk
        )
        copy.start()
        ins.append(copy)
    y0[block_rows(blk, rep), :] = (damped(rep) * scale[pl.ds(rep, 1), 0:1]).astype(bf16)

    def first_step(b, r):
        at = block_rows(b, r)
        ids = (b * reps + r) * rows + lax.broadcasted_iota(jnp.int32, (rows, order), 0)
        eye = ids == lax.broadcasted_iota(jnp.int32, (rows, order), 1)
        z1[at, :] = ((jnp.where(eye, 3.0, 0.0) - y0[at, :].astype(f32)) * 0.5).astype(bf16)

    forwards = []
    for k in range(reps):
        src = lax.rem(rep - k + reps, reps)
        if k:
            ins[k - 1].wait_recv()
        at = block_rows(blk, src)
        copy = remote(y0.at[at], y0.at[at], fwd_send.at[k], fwd_recv.at[k], rep, 1 - blk)
        copy.start()
        forwards.append(copy)
        first_step(blk, src)
    for k in range(reps):
        src = lax.rem(rep - k + reps, reps)
        forwards[k].wait_recv()
        first_step(1 - blk, src)

    mine = pl.ds(pl.multiple_of(blk * half, half), half)
    pending = []

    def cols(n):
        return slice(n * CHUNK, (n + 1) * CHUNK)

    def share(dst, ex, n):
        view = dst.at[mine, pl.ds(n * CHUNK, CHUNK)]
        copy = remote(view, view, ex_send.at[ex, n], ex_recv.at[ex, n], rep, 1 - blk)
        copy.start()
        pending.append(copy)
        return copy

    def product(lhs, rhs, arrivals, n):
        if arrivals is not None:
            arrivals[n].wait_recv()
        return jnp.dot(lhs, rhs[:, cols(n)], preferred_element_type=f32)

    def advance(lhs, rhs, arrivals, dst, ex):
        shared = []
        for n in range(chunks):
            dst[mine, cols(n)] = product(lhs[...], rhs, arrivals, n).astype(bf16)
            shared.append(share(dst, ex, n))
        return shared

    eye_rows = blk * half + lax.broadcasted_iota(jnp.int32, (half, CHUNK), 0)
    eye_cols = lax.broadcasted_iota(jnp.int32, (half, CHUNK), 1)

    def make_step(y, z, arrivals):
        for n in range(chunks):
            moment = product(y[mine, :], z, arrivals, n)
            eye = jnp.where(eye_rows == eye_cols + n * CHUNK, 3.0, 0.0)
            step[:, cols(n)] = ((eye - moment) * 0.5).astype(bf16)

    y, z, z_in = full.at[2], z1, None
    y_in = advance(z1.at[mine], y0, None, y, 0)
    slot, ex = 3, 1
    for _ in range(ITERS - 2):
        make_step(y, z, z_in)
        z_next, y_next = full.at[slot], full.at[slot + 1]
        z_in_next = advance(step, z, None, z_next, ex)
        y_in = advance(step, y, y_in, y_next, ex + 1)
        y, z, z_in = y_next, z_next, z_in_next
        slot, ex = slot + 2, ex + 2
    make_step(y, z, z_in)

    my_cols = pl.ds(pl.multiple_of(blk * half, LANES), half)
    for n in range(chunks):
        out = product(step[...], y, y_in, n)
        last_root[cols(n), :] = out.T.astype(bf16)
    roots = []
    for j in range(1, members):
        r, b = member(j)
        copy = remote(
            last_root.at[block_rows(b, r)], root_ref.at[rep, :, my_cols],
            root_send.at[j], root_recv.at[j], r, b,
        )
        copy.start()
        roots.append(copy)
    root_ref[rep, :, my_cols] = last_root[block_rows(blk, rep), :]

    for n in range(chunks):
        z1[0:half, cols(n)] = product(step[...], z, None, n).astype(bf16)

    def local_rows(r):
        return pl.ds(pl.multiple_of(r * rows, rows), rows)

    invs = []
    for k in range(1, reps):
        p = lax.rem(rep + k, reps)
        copy = remote(
            z1.at[local_rows(p)], inv_ref.at[rep], inv_send.at[k], inv_recv.at[k], p, blk
        )
        copy.start()
        invs.append(copy)
    inv_ref[rep] = z1[local_rows(rep), :]

    for copy in ins + forwards + pending:
        copy.wait_send()
    for copy in roots + invs:
        copy.wait()


def fused(mesh, factors, damping):
    facs, rows, order = factors.shape
    reps = mesh.shape["rep"]
    members = 2 * reps
    half = rows * reps
    chunks = order // CHUNK
    dma = pltpu.SemaphoreType.DMA
    vmem = pl.BlockSpec(memory_space=pltpu.VMEM)
    exchanges = 2 * ITERS - 3
    root, inv, norm = pl.pallas_call(
        functools.partial(kernel, reps),
        out_shape=(
            jax.ShapeDtypeStruct(factors.shape, jnp.bfloat16),
            jax.ShapeDtypeStruct(factors.shape, jnp.bfloat16),
            jax.ShapeDtypeStruct((facs, LANES), jnp.float32),
        ),
        in_specs=[
            pl.BlockSpec(memory_space=pl.ANY),
            pl.BlockSpec(memory_space=pltpu.SMEM),
        ],
        out_specs=(vmem, vmem, vmem),
        scratch_shapes=[
            pltpu.VMEM(factors.shape, jnp.float32),
            pltpu.VMEM((members, facs, LANES), jnp.float32),
            pltpu.VMEM((facs, LANES), jnp.float32),
            pltpu.VMEM(factors.shape, jnp.bfloat16),
            pltpu.VMEM((2 * ITERS - 1, order, order), jnp.bfloat16),
            pltpu.VMEM((half, order), jnp.bfloat16),
            pltpu.VMEM((order, half), jnp.bfloat16),
            dma((facs,)),
            dma((members,)), dma((members,)),
            dma((reps,)), dma((reps,)),
            dma((reps,)), dma((reps,)),
            dma((exchanges, chunks)), dma((exchanges, chunks)),
            dma((members,)), dma((members,)),
            dma((reps,)), dma((reps,)),
        ],
        compiler_params=pltpu.CompilerParams(
            collective_id=0, has_side_effects=True, vmem_limit_bytes=60 * 2**20
        ),
    )(factors, damping)
    root_scale = jnp.sqrt(norm[:, :1])[:, :, None]
    return root.astype(jnp.float32) * root_scale, inv.astype(jnp.float32) / root_scale


def plain(factors, damping):
    fac_grp, row_count, order_full = factors.shape
    rep_count = lax.axis_size("rep")
    fac_rep = fac_grp // rep_count
    blk_rows = row_count * rep_count
    blk_idx = lax.axis_index("blk")
    rep_idx = lax.axis_index("rep")
    row_ids = blk_idx * blk_rows + rep_idx * row_count + lax.iota(jnp.int32, row_count)
    col_ids = lax.iota(jnp.int32, order_full)
    eye_block = (row_ids[:, None] == col_ids[None, :]).astype(jnp.float32)
    damped = factors + damping[:, None, None] * eye_block[None, :, :]
    factor_norms = jnp.sqrt(lax.psum(jnp.sum(damped * damped, axis=(1, 2)), ("rep", "blk")))
    own_rows = lax.all_to_all(damped, "rep", split_axis=0, concat_axis=1, tiled=True)
    own_norms = lax.dynamic_slice_in_dim(factor_norms, rep_idx * fac_rep, fac_rep)
    iterate = (own_rows / own_norms[:, None, None]).astype(jnp.bfloat16)
    iter_rows = blk_idx * blk_rows + lax.iota(jnp.int32, blk_rows)
    eye_rows = (iter_rows[:, None] == col_ids[None, :]).astype(jnp.float32)
    inverse = eye_rows[None, :, :].astype(jnp.bfloat16)
    for _ in range(ITERS):
        whole_iter = lax.all_gather(iterate, "blk", axis=1, tiled=True)
        whole_inv = lax.all_gather(inverse, "blk", axis=1, tiled=True)
        eye_full = jnp.eye(order_full, dtype=jnp.float32)
        moment = jnp.einsum(
            "fik,fkj->fij", whole_inv, whole_iter, preferred_element_type=jnp.float32
        )
        step = ((3.0 * eye_full[None, :, :] - moment) * 0.5).astype(jnp.bfloat16)
        step_rows = lax.dynamic_slice_in_dim(step, blk_idx * blk_rows, blk_rows, 1)
        new_iterate = jnp.einsum("fik,fkj->fij", iterate, step, preferred_element_type=jnp.float32)
        new_inverse = jnp.einsum(
            "fik,fkj->fij", step_rows, whole_inv, preferred_element_type=jnp.float32
        )
        iterate = new_iterate.astype(jnp.bfloat16)
        inverse = new_inverse.astype(jnp.bfloat16)
    root = lax.all_to_all(iterate, "rep", split_axis=1, concat_axis=0, tiled=True)
    inv = lax.all_to_all(inverse, "rep", split_axis=1, concat_axis=0, tiled=True)
    root_scale = jnp.sqrt(factor_norms)[:, None, None]
    return root.astype(jnp.float32) * root_scale, inv.astype(jnp.float32) / root_scale


def solution(mesh):
    def per_device(factors, damping):
        facs, rows, order = factors.shape
        if (
            facs == mesh.shape["rep"]
            and mesh.shape["blk"] == 2
            and rows % 16 == 0
            and order % CHUNK == 0
        ):
            return fused(mesh, factors, damping)
        return plain(factors, damping)

    return jax.shard_map(
        per_device,
        mesh=mesh,
        in_specs=(P("grp", ("blk", "rep"), None), P("grp")),
        out_specs=(P("grp", ("blk", "rep"), None), P("grp", ("blk", "rep"), None)),
        check_vma=False,
    )
```

```python
import functools

import jax
import jax.numpy as jnp
from jax import lax
from jax.experimental import pallas as pl
from jax.experimental.pallas import tpu as pltpu
from jax.sharding import PartitionSpec as P

ITERS = 4
LANES = 128
CHUNK = 256
MESH = pl.DeviceIdType.MESH


def kernel(
    reps, fac_hbm, damp_ref,
    root_ref, inv_ref, norm_ref,
    fac, part, scale, send_buf, full, step, last_root,
    load_sem, sum_send, sum_recv, in_send, in_recv, fwd_send, fwd_recv,
    ex_send, ex_recv, root_send, root_recv, inv_send, inv_recv,
):
    grp = lax.axis_index("grp")
    rep = lax.axis_index("rep")
    blk = lax.axis_index("blk")
    facs, rows, order = fac.shape
    half = rows * reps
    members = 2 * reps
    rank = blk * reps + rep
    chunks = order // CHUNK
    f32, bf16 = jnp.float32, jnp.bfloat16

    def remote(src, dst, send, recv, r, b):
        return pltpu.make_async_remote_copy(
            src_ref=src, dst_ref=dst, send_sem=send, recv_sem=recv,
            device_id=(grp, r, b), device_id_type=MESH,
        )

    def member(j):
        q = lax.rem(rank + j, members)
        return lax.rem(q, reps), q // reps

    loads = [
        pltpu.make_async_copy(fac_hbm.at[f], fac.at[f], load_sem.at[f]) for f in range(facs)
    ]
    for load in loads:
        load.start()
    barrier = pltpu.get_barrier_semaphore()
    for j in range(1, members):
        r, b = member(j)
        pl.semaphore_signal(barrier, inc=1, device_id=(grp, r, b), device_id_type=MESH)

    row_ids = rank * rows + lax.broadcasted_iota(jnp.int32, (rows, order), 0)
    diag = row_ids == lax.broadcasted_iota(jnp.int32, (rows, order), 1)

    def damped(f):
        return fac[f] + jnp.where(diag, damp_ref[f], 0.0)

    for f in range(facs):
        loads[f].wait()
        x = damped(f)
        col = jnp.sum(x * x, axis=0, keepdims=True)
        acc = col[:, :LANES]
        for c in range(1, order // LANES):
            acc = acc + col[:, c * LANES : (c + 1) * LANES]
        part[pl.ds(rank, 1), f : f + 1, :] = acc[None]
    pl.semaphore_wait(barrier, members - 1)

    sums = []
    for j in range(1, members):
        r, b = member(j)
        copy = remote(part.at[rank], part.at[rank], sum_send.at[j], sum_recv.at[j], r, b)
        copy.start()
        sums.append(copy)
    for copy in sums:
        copy.wait()
    total = part[0]
    for q in range(1, members):
        total = total + part[q]
    norm = jnp.sqrt(jnp.sum(total, axis=1, keepdims=True))
    norm_ref[...] = jnp.broadcast_to(norm, norm_ref.shape)
    scale[...] = jnp.broadcast_to(1.0 / norm, scale.shape)

    y0, z1 = full.at[0], full.at[1]

    def block_rows(b, r):
        return pl.ds(pl.multiple_of((b * reps + r) * rows, rows), rows)

    side_reps = reps // 2
    side = rep // side_reps
    wide = -(-(half // 2) // LANES) * LANES
    narrow = half - wide

    def target(k):
        if k <= side_reps:
            return (1 - side) * side_reps + lax.rem(rep + k, side_reps)
        return side * side_reps + lax.rem(rep + k, side_reps)

    def source(k):
        if k == 0:
            return rep
        back = lax.rem(rep - k + reps, side_reps)
        if k <= side_reps:
            return (1 - side) * side_reps + back
        return side * side_reps + back

    def pieces(k, owner_side):
        if k == 0 or k > side_reps:
            return [pl.ds(0, order)]
        first = (1 - owner_side) * narrow
        return [
            pl.ds(pl.multiple_of(h * half + first, LANES), wide) for h in range(2)
        ]

    ins = []
    for k in range(1, reps):
        p = target(k)
        send_buf[k] = (damped(p) * scale[pl.ds(p, 1), 0:1]).astype(bf16)
        at = block_rows(blk, rep)
        copies = [
            remote(
                send_buf.at[k, :, c], y0.at[at, c],
                in_send.at[k, i], in_recv.at[k, i], p, blk,
            )
            for i, c in enumerate(pieces(k, 1 - side))
        ]
        for copy in copies:
            copy.start()
        ins.append(copies)
    y0[block_rows(blk, rep), :] = (damped(rep) * scale[pl.ds(rep, 1), 0:1]).astype(bf16)

    forwards = []
    for k in [0] + list(range(side_reps + 1, reps)) + list(range(1, side_reps + 1)):
        at = block_rows(blk, source(k))
        for i, c in enumerate(pieces(k, side)):
            if k:
                ins[k - 1][i].wait_recv()
            copy = remote(
                y0.at[at, c], y0.at[at, c], fwd_send.at[k, i], fwd_recv.at[k, i], rep, 1 - blk
            )
            copy.start()
            forwards.append(copy)
    for copy in forwards:
        copy.wait_recv()
    for copy in forwards:
        copy.wait_send()

    far = half // 2

    @pl.when(side == 0)
    def _():
        for hi in range(2):
            for hj in range(2):
                t = y0[hj * half : hj * half + narrow, hi * half + narrow : (hi + 1) * half]
                y0[hi * half + far : (hi + 1) * half, hj * half : hj * half + narrow] = (
                    t.astype(f32).T[far - narrow :, :].astype(bf16)
                )

    @pl.when(side == 1)
    def _():
        for hi in range(2):
            for hj in range(2):
                t = y0[hj * half + wide : (hj + 1) * half, hi * half : hi * half + wide]
                y0[hi * half : hi * half + far, hj * half + wide : (hj + 1) * half] = (
                    t.astype(f32).T[:far, :].astype(bf16)
                )

    for q in range(members):
        at = slice(q * rows, (q + 1) * rows)
        ids = q * rows + lax.broadcasted_iota(jnp.int32, (rows, order), 0)
        eye = ids == lax.broadcasted_iota(jnp.int32, (rows, order), 1)
        z1[at, :] = ((jnp.where(eye, 3.0, 0.0) - y0[at, :].astype(f32)) * 0.5).astype(bf16)

    mine = pl.ds(pl.multiple_of(blk * half, half), half)
    pending = []

    def cols(n):
        return slice(n * CHUNK, (n + 1) * CHUNK)

    def share(dst, ex, n):
        view = dst.at[mine, pl.ds(n * CHUNK, CHUNK)]
        copy = remote(view, view, ex_send.at[ex, n], ex_recv.at[ex, n], rep, 1 - blk)
        copy.start()
        pending.append(copy)
        return copy

    def product(lhs, rhs, arrivals, n):
        if arrivals is not None:
            arrivals[n].wait_recv()
        return jnp.dot(lhs, rhs[:, cols(n)], preferred_element_type=f32)

    def advance(lhs, rhs, arrivals, dst, ex):
        shared = []
        for n in range(chunks):
            dst[mine, cols(n)] = product(lhs[...], rhs, arrivals, n).astype(bf16)
            shared.append(share(dst, ex, n))
        return shared

    eye_rows = blk * half + lax.broadcasted_iota(jnp.int32, (half, CHUNK), 0)
    eye_cols = lax.broadcasted_iota(jnp.int32, (half, CHUNK), 1)

    def make_step(y, z, arrivals):
        for n in range(chunks):
            moment = product(y[mine, :], z, arrivals, n)
            eye = jnp.where(eye_rows == eye_cols + n * CHUNK, 3.0, 0.0)
            step[:, cols(n)] = ((eye - moment) * 0.5).astype(bf16)

    y, z, z_in = full.at[2], z1, None
    y_in = advance(z1.at[mine], y0, None, y, 0)
    slot, ex = 3, 1
    for _ in range(ITERS - 2):
        make_step(y, z, z_in)
        z_next, y_next = full.at[slot], full.at[slot + 1]
        z_in_next = advance(step, z, None, z_next, ex)
        y_in = advance(step, y, y_in, y_next, ex + 1)
        y, z, z_in = y_next, z_next, z_in_next
        slot, ex = slot + 2, ex + 2
    make_step(y, z, z_in)

    for n in range(chunks):
        z1[0:half, cols(n)] = product(step[...], z, None, n).astype(bf16)

    def local_rows(r):
        return pl.ds(pl.multiple_of(r * rows, rows), rows)

    invs = []
    for k in range(1, reps):
        p = target(k)
        copy = remote(
            z1.at[local_rows(p)], inv_ref.at[rep], inv_send.at[k], inv_recv.at[k], p, blk
        )
        copy.start()
        invs.append(copy)

    my_cols = pl.ds(pl.multiple_of(blk * half, LANES), half)
    for n in range(chunks):
        out = product(step[...], y, y_in, n)
        last_root[cols(n), :] = out.T.astype(bf16)
    roots = []
    for k in list(range(1, reps)) + [0]:
        for flip in range(2):
            if k == 0 and flip == 0:
                continue
            r = target(k) if k else rep
            b = blk + flip - 2 * blk * flip
            copy = remote(
                last_root.at[block_rows(b, r)], root_ref.at[rep, :, my_cols],
                root_send.at[k, flip], root_recv.at[k, flip], r, b,
            )
            copy.start()
            roots.append(copy)
    inv_ref[rep] = z1[local_rows(rep), :]
    root_ref[rep, :, my_cols] = last_root[block_rows(blk, rep), :]

    for copies in ins:
        for copy in copies:
            copy.wait_send()
    for copy in pending:
        copy.wait_send()
    for copy in invs + roots:
        copy.wait()


def fused(mesh, factors, damping):
    facs, rows, order = factors.shape
    reps = mesh.shape["rep"]
    members = 2 * reps
    half = rows * reps
    chunks = order // CHUNK
    dma = pltpu.SemaphoreType.DMA
    vmem = pl.BlockSpec(memory_space=pltpu.VMEM)
    exchanges = 2 * ITERS - 3
    root, inv, norm = pl.pallas_call(
        functools.partial(kernel, reps),
        out_shape=(
            jax.ShapeDtypeStruct(factors.shape, jnp.bfloat16),
            jax.ShapeDtypeStruct(factors.shape, jnp.bfloat16),
            jax.ShapeDtypeStruct((facs, LANES), jnp.float32),
        ),
        in_specs=[
            pl.BlockSpec(memory_space=pl.ANY),
            pl.BlockSpec(memory_space=pltpu.SMEM),
        ],
        out_specs=(vmem, vmem, vmem),
        scratch_shapes=[
            pltpu.VMEM(factors.shape, jnp.float32),
            pltpu.VMEM((members, facs, LANES), jnp.float32),
            pltpu.VMEM((facs, LANES), jnp.float32),
            pltpu.VMEM(factors.shape, jnp.bfloat16),
            pltpu.VMEM((2 * ITERS - 1, order, order), jnp.bfloat16),
            pltpu.VMEM((half, order), jnp.bfloat16),
            pltpu.VMEM((order, half), jnp.bfloat16),
            dma((facs,)),
            dma((members,)), dma((members,)),
            dma((reps, 2)), dma((reps, 2)),
            dma((reps, 2)), dma((reps, 2)),
            dma((exchanges, chunks)), dma((exchanges, chunks)),
            dma((reps, 2)), dma((reps, 2)),
            dma((reps,)), dma((reps,)),
        ],
        compiler_params=pltpu.CompilerParams(
            collective_id=0, has_side_effects=True, vmem_limit_bytes=60 * 2**20
        ),
    )(factors, damping)
    root_scale = jnp.sqrt(norm[:, :1])[:, :, None]
    return root.astype(jnp.float32) * root_scale, inv.astype(jnp.float32) / root_scale


def plain(factors, damping):
    fac_grp, row_count, order_full = factors.shape
    rep_count = lax.axis_size("rep")
    fac_rep = fac_grp // rep_count
    blk_rows = row_count * rep_count
    blk_idx = lax.axis_index("blk")
    rep_idx = lax.axis_index("rep")
    row_ids = blk_idx * blk_rows + rep_idx * row_count + lax.iota(jnp.int32, row_count)
    col_ids = lax.iota(jnp.int32, order_full)
    eye_block = (row_ids[:, None] == col_ids[None, :]).astype(jnp.float32)
    damped = factors + damping[:, None, None] * eye_block[None, :, :]
    factor_norms = jnp.sqrt(lax.psum(jnp.sum(damped * damped, axis=(1, 2)), ("rep", "blk")))
    own_rows = lax.all_to_all(damped, "rep", split_axis=0, concat_axis=1, tiled=True)
    own_norms = lax.dynamic_slice_in_dim(factor_norms, rep_idx * fac_rep, fac_rep)
    iterate = (own_rows / own_norms[:, None, None]).astype(jnp.bfloat16)
    iter_rows = blk_idx * blk_rows + lax.iota(jnp.int32, blk_rows)
    eye_rows = (iter_rows[:, None] == col_ids[None, :]).astype(jnp.float32)
    inverse = eye_rows[None, :, :].astype(jnp.bfloat16)
    for _ in range(ITERS):
        whole_iter = lax.all_gather(iterate, "blk", axis=1, tiled=True)
        whole_inv = lax.all_gather(inverse, "blk", axis=1, tiled=True)
        eye_full = jnp.eye(order_full, dtype=jnp.float32)
        moment = jnp.einsum(
            "fik,fkj->fij", whole_inv, whole_iter, preferred_element_type=jnp.float32
        )
        step = ((3.0 * eye_full[None, :, :] - moment) * 0.5).astype(jnp.bfloat16)
        step_rows = lax.dynamic_slice_in_dim(step, blk_idx * blk_rows, blk_rows, 1)
        new_iterate = jnp.einsum("fik,fkj->fij", iterate, step, preferred_element_type=jnp.float32)
        new_inverse = jnp.einsum(
            "fik,fkj->fij", step_rows, whole_inv, preferred_element_type=jnp.float32
        )
        iterate = new_iterate.astype(jnp.bfloat16)
        inverse = new_inverse.astype(jnp.bfloat16)
    root = lax.all_to_all(iterate, "rep", split_axis=1, concat_axis=0, tiled=True)
    inv = lax.all_to_all(inverse, "rep", split_axis=1, concat_axis=0, tiled=True)
    root_scale = jnp.sqrt(factor_norms)[:, None, None]
    return root.astype(jnp.float32) * root_scale, inv.astype(jnp.float32) / root_scale


def solution(mesh):
    def per_device(factors, damping):
        facs, rows, order = factors.shape
        if (
            facs == mesh.shape["rep"]
            and mesh.shape["blk"] == 2
            and rows % 16 == 0
            and facs % 2 == 0
            and (rows * facs) % LANES == 0
            and order % CHUNK == 0
        ):
            return fused(mesh, factors, damping)
        return plain(factors, damping)

    return jax.shard_map(
        per_device,
        mesh=mesh,
        in_specs=(P("grp", ("blk", "rep"), None), P("grp")),
        out_specs=(P("grp", ("blk", "rep"), None), P("grp", ("blk", "rep"), None)),
        check_vma=False,
    )
```

```python
import functools

import jax
import jax.numpy as jnp
from jax import lax
from jax.experimental import pallas as pl
from jax.experimental.pallas import tpu as pltpu
from jax.sharding import PartitionSpec as P

ITERS = 4
LANES = 128
CHUNK = 256
MESH = pl.DeviceIdType.MESH


def kernel(
    reps, fac_hbm, damp_ref,
    root_ref, inv_ref, norm_ref,
    fac, part, scale, send_buf, full, step, last_root,
    load_sem, sum_send, sum_recv, in_send, in_recv, fwd_send, fwd_recv,
    ex_send, ex_recv, root_send, root_recv, inv_send, inv_recv,
):
    grp = lax.axis_index("grp")
    rep = lax.axis_index("rep")
    blk = lax.axis_index("blk")
    facs, rows, order = fac.shape
    half = rows * reps
    members = 2 * reps
    rank = blk * reps + rep
    chunks = order // CHUNK
    f32, bf16 = jnp.float32, jnp.bfloat16

    def remote(src, dst, send, recv, r, b):
        return pltpu.make_async_remote_copy(
            src_ref=src, dst_ref=dst, send_sem=send, recv_sem=recv,
            device_id=(grp, r, b), device_id_type=MESH,
        )

    def member(j):
        q = lax.rem(rank + j, members)
        return lax.rem(q, reps), q // reps

    loads = [
        pltpu.make_async_copy(fac_hbm.at[f], fac.at[f], load_sem.at[f]) for f in range(facs)
    ]
    for load in loads:
        load.start()
    barrier = pltpu.get_barrier_semaphore()
    for j in range(1, members):
        r, b = member(j)
        pl.semaphore_signal(barrier, inc=1, device_id=(grp, r, b), device_id_type=MESH)

    row_ids = rank * rows + lax.broadcasted_iota(jnp.int32, (rows, order), 0)
    diag = row_ids == lax.broadcasted_iota(jnp.int32, (rows, order), 1)

    def damped(f):
        return fac[f] + jnp.where(diag, damp_ref[f], 0.0)

    for f in range(facs):
        loads[f].wait()
        x = damped(f)
        col = jnp.sum(x * x, axis=0, keepdims=True)
        acc = col[:, :LANES]
        for c in range(1, order // LANES):
            acc = acc + col[:, c * LANES : (c + 1) * LANES]
        part[pl.ds(rank, 1), f : f + 1, :] = acc[None]
    pl.semaphore_wait(barrier, members - 1)

    sums = []
    for j in range(1, members):
        r, b = member(j)
        copy = remote(part.at[rank], part.at[rank], sum_send.at[j], sum_recv.at[j], r, b)
        copy.start()
        sums.append(copy)
    for copy in sums:
        copy.wait()
    total = part[0]
    for q in range(1, members):
        total = total + part[q]
    norm = jnp.sqrt(jnp.sum(total, axis=1, keepdims=True))
    norm_ref[...] = jnp.broadcast_to(norm, norm_ref.shape)
    scale[...] = jnp.broadcast_to(1.0 / norm, scale.shape)

    y0, z1 = full.at[0], full.at[1]

    def block_rows(b, r):
        return pl.ds(pl.multiple_of((b * reps + r) * rows, rows), rows)

    side_reps = reps // 2
    side = rep // side_reps
    wide = -(-(half // 2) // LANES) * LANES
    narrow = half - wide

    def target(k):
        if k <= side_reps:
            return (1 - side) * side_reps + lax.rem(rep + k, side_reps)
        return side * side_reps + lax.rem(rep + k, side_reps)

    def source(k):
        if k == 0:
            return rep
        back = lax.rem(rep - k + reps, side_reps)
        if k <= side_reps:
            return (1 - side) * side_reps + back
        return side * side_reps + back

    tiles = half // LANES
    widths = sorted({tiles - (r * rows) // LANES for r in range(side_reps, reps)})

    def width_of(r, owner_side):
        mirrored = r + owner_side * (reps - 1 - 2 * r)
        return tiles - (mirrored * rows) // LANES

    def pieces(k, src, owner_side):
        if k == 0 or k > side_reps:
            return [(None, [pl.ds(0, order)])]
        options = []
        for w in widths:
            first = (1 - owner_side) * (half - w * LANES)
            options.append((
                width_of(src, owner_side) == w,
                [pl.ds(pl.multiple_of(h * half + first, LANES), w * LANES) for h in range(2)],
            ))
        return options

    def each(options, act):
        for condition, columns in options:
            if condition is None:
                act(columns)
            else:
                pl.when(condition)(functools.partial(act, columns))

    own_rows = block_rows(blk, rep)

    def in_copy(k, i, c):
        return remote(
            send_buf.at[k, :, c], y0.at[own_rows, c],
            in_send.at[k, i], in_recv.at[k, i], target(k), blk,
        )

    def send_in(k, columns):
        for i, c in enumerate(columns):
            in_copy(k, i, c).start()

    def wait_in(k, columns):
        for i, c in enumerate(columns):
            in_copy(k, i, c).wait_send()

    for k in range(1, reps):
        p = target(k)
        send_buf[k] = (damped(p) * scale[pl.ds(p, 1), 0:1]).astype(bf16)
        each(pieces(k, rep, 1 - side), functools.partial(send_in, k))
    y0[own_rows, :] = (damped(rep) * scale[pl.ds(rep, 1), 0:1]).astype(bf16)

    def forward_copy(k, i, c):
        at = block_rows(blk, source(k))
        return remote(
            y0.at[at, c], y0.at[at, c], fwd_send.at[k, i], fwd_recv.at[k, i], rep, 1 - blk
        )

    def forward(k, columns):
        for i, c in enumerate(columns):
            if k:
                in_copy(k, i, c).wait_recv()
            forward_copy(k, i, c).start()

    def wait_forward(k, columns):
        for i, c in enumerate(columns):
            forward_copy(k, i, c).wait()

    for k in [0] + list(range(side_reps + 1, reps)) + list(range(1, side_reps + 1)):
        each(pieces(k, source(k), side), functools.partial(forward, k))
    for k in range(reps):
        each(pieces(k, source(k), side), functools.partial(wait_forward, k))

    far = half // 2
    miss = half - min(widths) * LANES

    def fill(t, old, row0, col0, mirrored):
        shape = (far, miss)
        r = (row0 + lax.broadcasted_iota(jnp.int32, shape, 0)) // rows
        c = (col0 + lax.broadcasted_iota(jnp.int32, shape, 1)) // LANES
        if mirrored:
            gone = c >= tiles - ((reps - 1 - r) * rows) // LANES
        else:
            gone = c < (r * rows) // LANES
        return jnp.where(gone, t, old.astype(f32)).astype(bf16)

    @pl.when(side == 0)
    def _():
        for hi in range(2):
            for hj in range(2):
                t = y0[hj * half : hj * half + miss, hi * half + narrow : (hi + 1) * half]
                at = (slice(hi * half + far, (hi + 1) * half), slice(hj * half, hj * half + miss))
                t = t.astype(f32).T[far - narrow :, :]
                y0[at] = fill(t, y0[at], far, 0, False)

    @pl.when(side == 1)
    def _():
        for hi in range(2):
            for hj in range(2):
                t = y0[(hj + 1) * half - miss : (hj + 1) * half, hi * half : hi * half + wide]
                at = (slice(hi * half, hi * half + far), slice((hj + 1) * half - miss, (hj + 1) * half))
                t = t.astype(f32).T[:far, :]
                y0[at] = fill(t, y0[at], 0, half - miss, True)

    for q in range(members):
        at = slice(q * rows, (q + 1) * rows)
        ids = q * rows + lax.broadcasted_iota(jnp.int32, (rows, order), 0)
        eye = ids == lax.broadcasted_iota(jnp.int32, (rows, order), 1)
        z1[at, :] = ((jnp.where(eye, 3.0, 0.0) - y0[at, :].astype(f32)) * 0.5).astype(bf16)

    mine = pl.ds(pl.multiple_of(blk * half, half), half)
    pending = []

    def cols(n):
        return slice(n * CHUNK, (n + 1) * CHUNK)

    def share(dst, ex, n):
        view = dst.at[mine, pl.ds(n * CHUNK, CHUNK)]
        copy = remote(view, view, ex_send.at[ex, n], ex_recv.at[ex, n], rep, 1 - blk)
        copy.start()
        pending.append(copy)
        return copy

    def product(lhs, rhs, arrivals, n):
        if arrivals is not None:
            arrivals[n].wait_recv()
        return jnp.dot(lhs, rhs[:, cols(n)], preferred_element_type=f32)

    def advance(lhs, rhs, arrivals, dst, ex):
        shared = []
        for n in range(chunks):
            dst[mine, cols(n)] = product(lhs[...], rhs, arrivals, n).astype(bf16)
            shared.append(share(dst, ex, n))
        return shared

    eye_rows = blk * half + lax.broadcasted_iota(jnp.int32, (half, CHUNK), 0)
    eye_cols = lax.broadcasted_iota(jnp.int32, (half, CHUNK), 1)

    def make_step(y, z, arrivals):
        for n in range(chunks):
            moment = product(y[mine, :], z, arrivals, n)
            eye = jnp.where(eye_rows == eye_cols + n * CHUNK, 3.0, 0.0)
            step[:, cols(n)] = ((eye - moment) * 0.5).astype(bf16)

    y, z, z_in = full.at[2], z1, None
    y_in = advance(z1.at[mine], y0, None, y, 0)
    slot, ex = 3, 1
    for _ in range(ITERS - 2):
        make_step(y, z, z_in)
        z_next, y_next = full.at[slot], full.at[slot + 1]
        z_in_next = advance(step, z, None, z_next, ex)
        y_in = advance(step, y, y_in, y_next, ex + 1)
        y, z, z_in = y_next, z_next, z_in_next
        slot, ex = slot + 2, ex + 2
    make_step(y, z, z_in)

    for n in range(chunks):
        z1[0:half, cols(n)] = product(step[...], z, None, n).astype(bf16)

    def local_rows(r):
        return pl.ds(pl.multiple_of(r * rows, rows), rows)

    invs = []
    for k in range(1, reps):
        p = target(k)
        copy = remote(
            z1.at[local_rows(p)], inv_ref.at[rep], inv_send.at[k], inv_recv.at[k], p, blk
        )
        copy.start()
        invs.append(copy)

    my_cols = pl.ds(pl.multiple_of(blk * half, LANES), half)
    for n in range(chunks):
        out = product(step[...], y, y_in, n)
        last_root[cols(n), :] = out.T.astype(bf16)
    roots = []
    for k in list(range(1, reps)) + [0]:
        for flip in range(2):
            if k == 0 and flip == 0:
                continue
            r = target(k) if k else rep
            b = blk + flip - 2 * blk * flip
            copy = remote(
                last_root.at[block_rows(b, r)], root_ref.at[rep, :, my_cols],
                root_send.at[k, flip], root_recv.at[k, flip], r, b,
            )
            copy.start()
            roots.append(copy)
    inv_ref[rep] = z1[local_rows(rep), :]
    root_ref[rep, :, my_cols] = last_root[block_rows(blk, rep), :]

    for k in range(1, reps):
        each(pieces(k, rep, 1 - side), functools.partial(wait_in, k))
    for copy in pending:
        copy.wait_send()
    for copy in invs + roots:
        copy.wait()


def fused(mesh, factors, damping):
    facs, rows, order = factors.shape
    reps = mesh.shape["rep"]
    members = 2 * reps
    half = rows * reps
    chunks = order // CHUNK
    dma = pltpu.SemaphoreType.DMA
    vmem = pl.BlockSpec(memory_space=pltpu.VMEM)
    exchanges = 2 * ITERS - 3
    root, inv, norm = pl.pallas_call(
        functools.partial(kernel, reps),
        out_shape=(
            jax.ShapeDtypeStruct(factors.shape, jnp.bfloat16),
            jax.ShapeDtypeStruct(factors.shape, jnp.bfloat16),
            jax.ShapeDtypeStruct((facs, LANES), jnp.float32),
        ),
        in_specs=[
            pl.BlockSpec(memory_space=pl.ANY),
            pl.BlockSpec(memory_space=pltpu.SMEM),
        ],
        out_specs=(vmem, vmem, vmem),
        scratch_shapes=[
            pltpu.VMEM(factors.shape, jnp.float32),
            pltpu.VMEM((members, facs, LANES), jnp.float32),
            pltpu.VMEM((facs, LANES), jnp.float32),
            pltpu.VMEM(factors.shape, jnp.bfloat16),
            pltpu.VMEM((2 * ITERS - 1, order, order), jnp.bfloat16),
            pltpu.VMEM((half, order), jnp.bfloat16),
            pltpu.VMEM((order, half), jnp.bfloat16),
            dma((facs,)),
            dma((members,)), dma((members,)),
            dma((reps, 2)), dma((reps, 2)),
            dma((reps, 2)), dma((reps, 2)),
            dma((exchanges, chunks)), dma((exchanges, chunks)),
            dma((reps, 2)), dma((reps, 2)),
            dma((reps,)), dma((reps,)),
        ],
        compiler_params=pltpu.CompilerParams(
            collective_id=0, has_side_effects=True, vmem_limit_bytes=60 * 2**20
        ),
    )(factors, damping)
    root_scale = jnp.sqrt(norm[:, :1])[:, :, None]
    return root.astype(jnp.float32) * root_scale, inv.astype(jnp.float32) / root_scale


def plain(factors, damping):
    fac_grp, row_count, order_full = factors.shape
    rep_count = lax.axis_size("rep")
    fac_rep = fac_grp // rep_count
    blk_rows = row_count * rep_count
    blk_idx = lax.axis_index("blk")
    rep_idx = lax.axis_index("rep")
    row_ids = blk_idx * blk_rows + rep_idx * row_count + lax.iota(jnp.int32, row_count)
    col_ids = lax.iota(jnp.int32, order_full)
    eye_block = (row_ids[:, None] == col_ids[None, :]).astype(jnp.float32)
    damped = factors + damping[:, None, None] * eye_block[None, :, :]
    factor_norms = jnp.sqrt(lax.psum(jnp.sum(damped * damped, axis=(1, 2)), ("rep", "blk")))
    own_rows = lax.all_to_all(damped, "rep", split_axis=0, concat_axis=1, tiled=True)
    own_norms = lax.dynamic_slice_in_dim(factor_norms, rep_idx * fac_rep, fac_rep)
    iterate = (own_rows / own_norms[:, None, None]).astype(jnp.bfloat16)
    iter_rows = blk_idx * blk_rows + lax.iota(jnp.int32, blk_rows)
    eye_rows = (iter_rows[:, None] == col_ids[None, :]).astype(jnp.float32)
    inverse = eye_rows[None, :, :].astype(jnp.bfloat16)
    for _ in range(ITERS):
        whole_iter = lax.all_gather(iterate, "blk", axis=1, tiled=True)
        whole_inv = lax.all_gather(inverse, "blk", axis=1, tiled=True)
        eye_full = jnp.eye(order_full, dtype=jnp.float32)
        moment = jnp.einsum(
            "fik,fkj->fij", whole_inv, whole_iter, preferred_element_type=jnp.float32
        )
        step = ((3.0 * eye_full[None, :, :] - moment) * 0.5).astype(jnp.bfloat16)
        step_rows = lax.dynamic_slice_in_dim(step, blk_idx * blk_rows, blk_rows, 1)
        new_iterate = jnp.einsum("fik,fkj->fij", iterate, step, preferred_element_type=jnp.float32)
        new_inverse = jnp.einsum(
            "fik,fkj->fij", step_rows, whole_inv, preferred_element_type=jnp.float32
        )
        iterate = new_iterate.astype(jnp.bfloat16)
        inverse = new_inverse.astype(jnp.bfloat16)
    root = lax.all_to_all(iterate, "rep", split_axis=1, concat_axis=0, tiled=True)
    inv = lax.all_to_all(inverse, "rep", split_axis=1, concat_axis=0, tiled=True)
    root_scale = jnp.sqrt(factor_norms)[:, None, None]
    return root.astype(jnp.float32) * root_scale, inv.astype(jnp.float32) / root_scale


def solution(mesh):
    def per_device(factors, damping):
        facs, rows, order = factors.shape
        if (
            facs == mesh.shape["rep"]
            and mesh.shape["blk"] == 2
            and rows % 16 == 0
            and facs % 2 == 0
            and (rows * facs) % LANES == 0
            and order % CHUNK == 0
        ):
            return fused(mesh, factors, damping)
        return plain(factors, damping)

    return jax.shard_map(
        per_device,
        mesh=mesh,
        in_specs=(P("grp", ("blk", "rep"), None), P("grp")),
        out_specs=(P("grp", ("blk", "rep"), None), P("grp", ("blk", "rep"), None)),
        check_vma=False,
    )
```
